32 devices in a mesh: gx: 2 (over x), gy: 4 (over y, core), gz: 4 (over z).
Axes of the slice: x: 2, y: 2, z: 4, core: 2. Of those that a mesh axis runs over, the one named last changes fastest.
Arguments:
- images: bfloat16 [32, 5, 524288], P(('gx', 'gy', 'gz')), may hold values from 0 to 0.125
- order: int32 [32], replicated, may hold values from 0 to 31, as said below
Outputs:
- frame: float32 [5, 524288], P(None, 'gx')
The draws below stay inside these ranges and needn't reach their ends.
Inputs may be any that keep to these rules, and one draw needn't show every extreme that they name: order is a permutation of the bricks, where brick r sits at index r // 16 along gx, (r // 4) % 4 along gy and r % 4 along gz; the bricks of one gz index take consecutive places, within them the bricks of one (gy, gz) pair take consecutive places; the order of gz indices, the order of gy indices within each gz index and the order of gx indices within each (gy, gz) pair are arbitrary and may differ from slab to slab and from column to column.
All inputs are finite; a program needn't handle non-finite values.
Results may differ from the reference program's by a relative error of at most 0.0003.
Values may be sent and summed in bfloat16 or wider, within the bound.
A program may use at most 64 MiB of HBM per device.

```python
import jax
import jax.numpy as jnp
from jax import lax

CHANNELS = 5
RANKS = 32
PIXELS = 524288
N_GX = 2
N_GY = 4
N_GZ = 4


def random_places(key, shape, count):
    scores = jax.random.randint(key, shape + (count,), 0, 1 << 20, dtype=jnp.int32)
    scores = scores * count + jnp.arange(count, dtype=jnp.int32)
    ranked = jnp.argsort(scores, axis=-1)
    return jnp.argsort(ranked, axis=-1).astype(jnp.int32)


def draw_order(key, part):
    place_z = random_places(jax.random.fold_in(key, 11), (), N_GZ)
    place_y = random_places(jax.random.fold_in(key, 13), (N_GZ,), N_GY)
    place_x = random_places(jax.random.fold_in(key, 17), (N_GY, N_GZ), N_GX)
    slab = place_z[None, None, :]
    column = jnp.transpose(place_y, (1, 0))[None, :, :]
    within = jnp.transpose(place_x, (2, 0, 1))
    grid = slab * (N_GY * N_GX) + column * N_GX + within
    return grid.reshape(-1).astype(jnp.int32)


def levels(own_key, extent, split, least, largest):
    gain = 1.0
    for axis_at, shards_of in split:
        steps = jax.random.uniform(jax.random.fold_in(jax.random.fold_in(own_key, 6), axis_at), (shards_of,), jnp.float32, least / len(split), largest / len(split))
        gain = gain * jnp.repeat(jnp.exp(steps), extent[axis_at] // shards_of).reshape((-1,) + (1,) * (len(extent) - 1 - axis_at))
    return gain


def setup_inputs(seed: int = 0) -> dict:
    keys = jax.random.split(jax.random.key(seed), 3)
    return {
        "images": jnp.clip(0.125 * jax.random.uniform(keys[0], (RANKS, CHANNELS, PIXELS), jnp.float32) ** levels(keys[0], (RANKS, CHANNELS, PIXELS), ((0, 32),), -0.2, 0.2), 0.0, 0.125).astype(jnp.bfloat16),
        "order": draw_order(jax.random.fold_in(keys[2], 71), 0),
    }


def reference(images, order):
    places = jnp.arange(RANKS, dtype=jnp.int32)
    brick = jnp.zeros((RANKS,), jnp.int32).at[order.astype(jnp.int32)].set(places)

    def layer(total, member):
        picture = lax.dynamic_index_in_dim(images, member, 0, keepdims=False).astype(jnp.float32)
        return total + (1.0 - total[4:5]) * picture, None

    start = jnp.zeros((images.shape[1], images.shape[2]), jnp.float32)
    total, _ = lax.scan(layer, start, brick)
    return total
```

```python
import functools

import jax
import jax.numpy as jnp
from jax import lax
from jax.experimental import pallas as pl
from jax.experimental.pallas import tpu as pltpu
from jax.sharding import PartitionSpec as P

MESH = pl.DeviceIdType.MESH
AXES = ("gx", "gy", "gz")
CHUNKS = 8


def span(start, size):
    return pl.ds(pl.multiple_of(start, 128), size)


def front_flags(keys):
    return [[None if i == j else jnp.where(a < b, 1.0, 0.0) for j, b in enumerate(keys)] for i, a in enumerate(keys)]


def blend(pictures, flags):
    alphas = [p[4:5] for p in pictures]
    total = None
    for j, picture in enumerate(pictures):
        clear = None
        for i, alpha in enumerate(alphas):
            if i != j:
                factor = 1.0 - flags[i][j] * alpha
                clear = factor if clear is None else clear * factor
        term = picture if clear is None else clear * picture
        total = term if total is None else total + term
    return total


def kernel(counts, chunks, order_ref, images_ref, out_ref, own, near, pair, side, slab, deep, done,
           load_sem, s1, r1, s2, r2, s3, r3, s4, r4, s5, r5, put_sem):
    nx, ny, nz = counts
    x, y, z = (lax.axis_index(a) for a in AXES)
    band = out_ref.shape[1]
    size = band // chunks
    strip = size // ny
    tile = strip // nz

    barrier = pltpu.get_barrier_semaphore()
    greeted = 0
    for name, me, n in zip(AXES, (x, y, z), counts):
        for d in range(1, n):
            pl.semaphore_signal(barrier, inc=1, device_id={name: lax.rem(me + d, n)}, device_id_type=MESH)
            greeted += 1
    loads = [
        pltpu.make_async_copy(
            images_ref.at[0, :, span(x * band + k * size, size)], own.at[:, span(k * size, size)], load_sem.at[k])
        for k in range(chunks)
    ]
    for c in loads:
        c.start()
    pl.semaphore_wait(barrier, greeted)

    def remote(src, dst, send, recv, name, peer):
        return pltpu.make_async_remote_copy(
            src_ref=src, dst_ref=dst, send_sem=send, recv_sem=recv, device_id={name: peer}, device_id_type=MESH)

    def behind(me, d, n):
        return lax.rem(me + n - d, n)

    def place(px, py, pz):
        return order_ref[(px * ny + py) * nz + pz]

    flags_x = front_flags([place(behind(x, d, nx), y, z) for d in range(nx)])
    flags_y = front_flags([place(0, behind(y, d, ny), z) for d in range(ny)])
    flags_z = front_flags([place(0, 0, behind(z, d, nz)) for d in range(nz)])

    first, second, third, fourth, fifth = {}, {}, {}, {}, {}
    for k in range(chunks):
        for d in range(1, nx):
            peer = lax.rem(x + d, nx)
            c = remote(images_ref.at[0, :, span(peer * band + k * size, size)],
                       near.at[d - 1, :, span(k * size, size)], s1.at[k, d - 1], r1.at[k, d - 1], "gx", peer)
            c.start()
            first[k, d] = c

    def sweep(total, body):
        step = min(total, 1024)

        @pl.loop(0, total // step)
        def _(i):
            body(i * step, step)

    def stage_pair(k):
        loads[k].wait()
        for d in range(1, nx):
            first[k, d].wait_recv()

        def body(at, step):
            here = span(k * size + at, step)
            pictures = [own[:, here].astype(jnp.float32)]
            pictures += [near[d - 1, :, here].astype(jnp.float32) for d in range(1, nx)]
            pair[:, here] = blend(pictures, flags_x)

        sweep(size, body)
        for d in range(1, ny):
            peer = lax.rem(y + d, ny)
            c = remote(pair.at[:, span(k * size + peer * strip, strip)],
                       side.at[d - 1, :, span(k * strip, strip)], s2.at[k, d - 1], r2.at[k, d - 1], "gy", peer)
            c.start()
            second[k, d] = c

    def stage_slab(k):
        for d in range(1, ny):
            second[k, d].wait_recv()

        def body(at, step):
            here = span(k * strip + at, step)
            pictures = [pair[:, span(k * size + y * strip + at, step)]]
            pictures += [side[d - 1, :, here] for d in range(1, ny)]
            slab[:, here] = blend(pictures, flags_y)

        sweep(strip, body)
        for d in range(1, nz):
            peer = lax.rem(z + d, nz)
            c = remote(slab.at[:, span(k * strip + peer * tile, tile)],
                       deep.at[d - 1, :, span(k * tile, tile)], s3.at[k, d - 1], r3.at[k, d - 1], "gz", peer)
            c.start()
            third[k, d] = c

    def stage_tile(k):
        for d in range(1, nz):
            third[k, d].wait_recv()

        def body(at, step):
            here = span(k * tile + at, step)
            pictures = [slab[:, span(k * strip + z * tile + at, step)]]
            pictures += [deep[d - 1, :, here] for d in range(1, nz)]
            done[:, here] = blend(pictures, flags_z)

        sweep(tile, body)
        here = done.at[:, span(k * tile, tile)]
        there = out_ref.at[:, span(k * size + y * strip + z * tile, tile)]
        put = pltpu.make_async_copy(here, there, put_sem.at[k])
        put.start()
        fourth[k, 0] = put
        for d in range(1, nz):
            c = remote(here, there, s4.at[k, d - 1], r4.at[k, d - 1], "gz", lax.rem(z + d, nz))
            c.start()
            fourth[k, d] = c

    bits = [1 << b for b in reversed(range((ny - 1).bit_length()))]

    def stage_spread(k, at):
        if at == 0:
            fourth[k, 0].wait()
            for d in range(1, nz):
                fourth[k, d].wait_recv()
            held = [0]
        else:
            held = [0]
            for b in bits[:at]:
                held += [m | b for m in held]
            for m in held:
                if m & bits[at - 1]:
                    fifth[k, m].wait_recv()
        if at == len(bits):
            return
        for m in held:
            where = out_ref.at[:, span(k * size + (y ^ m) * strip, strip)]
            arrives = m | bits[at]
            c = remote(where, where, s5.at[k, arrives - 1], r5.at[k, arrives - 1], "gy", y ^ bits[at])
            c.start()
            fifth[k, arrives] = c

    stages = [stage_pair, stage_slab, stage_tile]
    stages += [functools.partial(stage_spread, at=at) for at in range(len(bits) + 1)]
    for t in range(chunks + len(stages) - 1):
        for lag, stage in enumerate(stages):
            if 0 <= t - lag < chunks:
                stage(t - lag)
    for group in (first, second, third, fourth, fifth):
        for (k, d), c in group.items():
            if d:
                c.wait_send()


def per_device(counts, images, order):
    nx, ny, nz = counts
    channels, pixels = images.shape[1:]
    band = pixels // nx
    chunks = min(CHUNKS, band // (ny * nz * 128))
    f32, dma = jnp.float32, pltpu.SemaphoreType.DMA
    return pl.pallas_call(
        functools.partial(kernel, counts, chunks),
        out_shape=jax.ShapeDtypeStruct((channels, band), f32),
        in_specs=[pl.BlockSpec(memory_space=pltpu.SMEM), pl.BlockSpec(memory_space=pl.ANY)],
        out_specs=pl.BlockSpec(memory_space=pl.ANY),
        scratch_shapes=[
            pltpu.VMEM((channels, band), images.dtype),
            pltpu.VMEM((nx - 1, channels, band), images.dtype),
            pltpu.VMEM((channels, band), f32),
            pltpu.VMEM((ny - 1, channels, band // ny), f32),
            pltpu.VMEM((channels, band // ny), f32),
            pltpu.VMEM((nz - 1, channels, band // (ny * nz)), f32),
            pltpu.VMEM((channels, band // (ny * nz)), f32),
            dma((chunks,)),
            dma((chunks, nx - 1)), dma((chunks, nx - 1)),
            dma((chunks, ny - 1)), dma((chunks, ny - 1)),
            dma((chunks, nz - 1)), dma((chunks, nz - 1)),
            dma((chunks, nz - 1)), dma((chunks, nz - 1)),
            dma((chunks, ny - 1)), dma((chunks, ny - 1)),
            dma((chunks,)),
        ],
        compiler_params=pltpu.CompilerParams(
            collective_id=0, has_side_effects=True, vmem_limit_bytes=60 * 1024 * 1024),
    )(order, images)


def solution(mesh):
    counts = tuple(mesh.shape[a] for a in AXES)
    return jax.shard_map(
        functools.partial(per_device, counts), mesh=mesh,
        in_specs=(P(AXES, None, None), P()), out_specs=P(None, "gx"), check_vma=False)
```

```python
import functools

import jax
import jax.numpy as jnp
from jax import lax
from jax.experimental import pallas as pl
from jax.experimental.pallas import tpu as pltpu
from jax.sharding import PartitionSpec as P

MESH = pl.DeviceIdType.MESH
AXES = ("gx", "gy", "gz")
CHUNKS = 8
PLANS = (0,)


LANES = 128
GROUP = 16


def span(start, size, unit):
    return pl.ds(pl.multiple_of(start, unit), size)


def front_flags(keys):
    return [[None if i == j else jnp.where(a < b, 1.0, 0.0) for j, b in enumerate(keys)] for i, a in enumerate(keys)]


def blend(pictures, flags):
    alphas = [p[4] for p in pictures]
    total = None
    for j, picture in enumerate(pictures):
        clear = None
        for i, alpha in enumerate(alphas):
            if i != j:
                factor = 1.0 - flags[i][j] * alpha
                clear = factor if clear is None else clear * factor
        term = picture if clear is None else [clear * c for c in picture]
        total = term if total is None else [t + c for t, c in zip(total, term)]
    return total


def kernel(counts, chunks, order_ref, images_ref, out_ref, raw, sent, near, pair, side, slab, deep, done, turn,
           load_sem, s1, r1, s2, r2, s3, r3, s4, r4, put_sem):
    nx, ny, nz = counts
    x, y, z = (lax.axis_index(a) for a in AXES)
    channels = out_ref.shape[0]
    band = out_ref.shape[1]
    size = band // chunks
    strip = size // ny
    tile = strip // nz
    f32 = jnp.float32

    barrier = pltpu.get_barrier_semaphore()
    greeted = 0
    for name, me, n in zip(AXES, (x, y, z), counts):
        for d in range(1, n):
            pl.semaphore_signal(barrier, inc=1, device_id={name: lax.rem(me + d, n)}, device_id_type=MESH)
            greeted += 1
    loads = {}
    for k in range(chunks):
        for d in [*range(1, nx), 0]:
            whose = lax.rem(x + d, nx)
            loads[k, d] = pltpu.make_async_copy(
                images_ref.at[0, :, span((whose * band + k * size) * LANES, size * LANES, LANES)],
                raw.at[d, :, span(k * size * LANES, size * LANES, LANES)], load_sem.at[k, d])
            loads[k, d].start()
    pl.semaphore_wait(barrier, greeted)

    def remote(src, dst, send, recv, name, peer):
        return pltpu.make_async_remote_copy(
            src_ref=src, dst_ref=dst, send_sem=send, recv_sem=recv, device_id={name: peer}, device_id_type=MESH)

    def behind(me, d, n):
        return lax.rem(me + n - d, n)

    def place(px, py, pz):
        return order_ref[(px * ny + py) * nz + pz]

    flags_x = front_flags([place(behind(x, d, nx), y, z) for d in range(nx)])
    flags_y = front_flags([place(0, behind(y, d, ny), z) for d in range(ny)])
    flags_z = front_flags([place(0, 0, behind(z, d, nz)) for d in range(nz)])
    first, second, third, gathered = {}, {}, {}, {}

    def sweep(total, step, body, unroll=1):
        lax.fori_loop(0, total // step, lambda i, _: (body(i * step), 0)[1], 0, unroll=unroll)

    def spread_rows(k, d):
        def body(at):
            value = raw[d, :, span((k * size + at) * LANES, 8 * LANES, LANES)].astype(f32)
            for t in range(8):
                turn[span((at + t) * 8, channels, 8), :] = value[:, t * LANES:(t + 1) * LANES]
        sweep(size, 8, body, 2)

    def turned(at, rows):
        return [
            jnp.concatenate([turn[pl.ds((at + r) * 8 + c, 8, stride=8), :] for r in range(0, rows, 8)], axis=0)
            for c in range(channels)
        ]

    def stage_send(k):
        for d in range(1, nx):
            loads[k, d].wait()
            spread_rows(k, d)

            def body(at):
                for c, value in enumerate(turned(at, GROUP)):
                    sent[d - 1, c, span(k * size + at, GROUP, GROUP), :] = value.astype(sent.dtype)
            sweep(size, GROUP, body, 2)
            here = span(k * size, size, GROUP)
            first[k, d] = remote(sent.at[d - 1, :, here], near.at[d - 1, :, here],
                                 s1.at[k, d - 1], r1.at[k, d - 1], "gx", lax.rem(x + d, nx))
            first[k, d].start()

    def stage_pair(k):
        loads[k, 0].wait()
        spread_rows(k, 0)
        for d in range(1, nx):
            first[k, d].wait_recv()

        def body(at):
            here = span(k * size + at, GROUP, GROUP)
            pictures = [turned(at, GROUP)]
            pictures += [[near[d - 1, c, here, :].astype(f32) for c in range(channels)] for d in range(1, nx)]
            for c, value in enumerate(blend(pictures, flags_x)):
                pair[c, here, :] = value
        sweep(size, GROUP, body)
        for d in range(1, ny):
            peer = lax.rem(y + d, ny)
            second[k, d] = remote(pair.at[:, span(k * size + peer * strip, strip, 8), :],
                                  side.at[d - 1, :, span(k * strip, strip, 8), :],
                                  s2.at[k, d - 1], r2.at[k, d - 1], "gy", peer)
            second[k, d].start()

    def stage_slab(k):
        for d in range(1, ny):
            second[k, d].wait_recv()

        def body(at):
            here = span(k * strip + at, 8, 8)
            pictures = [[pair[c, span(k * size + y * strip + at, 8, 8), :] for c in range(channels)]]
            pictures += [[side[d - 1, c, here, :] for c in range(channels)] for d in range(1, ny)]
            for c, value in enumerate(blend(pictures, flags_y)):
                slab[c, here, :] = value
        sweep(strip, 8, body)
        for d in range(1, nz):
            peer = lax.rem(z + d, nz)
            third[k, d] = remote(slab.at[:, span(k * strip + peer * tile, tile, 8), :],
                                 deep.at[d - 1, :, span(k * tile, tile, 8), :],
                                 s3.at[k, d - 1], r3.at[k, d - 1], "gz", peer)
            third[k, d].start()

    puts = {}

    def stage_tile(k):
        for d in range(1, nz):
            third[k, d].wait_recv()

        def body(at):
            here = span(k * tile + at, 8, 8)
            pictures = [[slab[c, span(k * strip + z * tile + at, 8, 8), :] for c in range(channels)]]
            pictures += [[deep[d - 1, c, here, :] for c in range(channels)] for d in range(1, nz)]
            for c, value in enumerate(blend(pictures, flags_z)):
                done[c, here, :] = value
        sweep(tile, 8, body)
        puts[k] = pltpu.make_async_copy(
            done.at[:, span(k * tile, tile, 8), :],
            out_ref.at[:, span(k * size + y * strip + z * tile, tile, 8), :], put_sem.at[k])
        puts[k].start()
        gather(k, 0)

    bits = [1 << b for b in reversed(range((ny - 1).bit_length()))]
    plans = [["z", *bits], [*bits[:1], "z", *bits[1:]]]

    def gather(k, at):
        plan = plans[PLANS[k % len(PLANS)]]
        masks, wide = [0], False
        for step in plan[:at]:
            if step == "z":
                wide = True
            else:
                masks += [m | step for m in masks]
        if at:
            for (kk, step, *name), c in list(gathered.items()):
                if kk == k and step == at - 1:
                    c.wait_recv()
        if at == len(plan):
            return
        step = plan[at]

        def slot(m, d):
            return m * nz + d
        for m in masks:
            base = k * size + (y ^ m) * strip
            if step == "z":
                ref = out_ref.at[:, span(base + z * tile, tile, 8), :]
                src = done.at[:, span(k * tile, tile, 8), :] if m == 0 else ref
                for d in range(1, nz):
                    c = remote(src, ref, s4.at[k, slot(m, d)], r4.at[k, slot(m, d)], "gz", lax.rem(z + d, nz))
                    c.start()
                    gathered[k, at, m, d] = c
            else:
                if wide:
                    if k in puts:
                        puts.pop(k).wait()
                    ref = src = out_ref.at[:, span(base, strip, 8), :]
                else:
                    ref = out_ref.at[:, span(base + z * tile, tile, 8), :]
                    src = done.at[:, span(k * tile, tile, 8), :] if m == 0 else ref
                n = slot(m | step, 0)
                c = remote(src, ref, s4.at[k, n], r4.at[k, n], "gy", y ^ step)
                c.start()
                gathered[k, at, m, 0] = c

    steps = len(bits) + 1
    stages = [stage_send, stage_pair, stage_slab, stage_tile]
    stages += [functools.partial(gather, at=at) for at in range(1, steps + 1)]
    lags = list(range(len(stages)))
    for t in range(chunks + lags[-1]):
        for lag, stage in zip(lags, stages):
            if 0 <= t - lag < chunks:
                stage(t - lag)
    for c in puts.values():
        c.wait()
    for group in (first, second, third, gathered):
        for c in group.values():
            c.wait_send()


def per_device(counts, images, order):
    nx, ny, nz = counts
    channels, pixels = images.shape[1:]
    band = pixels // nx // LANES
    chunks = min(CHUNKS, band // (ny * nz * 8))
    f32, dma = jnp.float32, pltpu.SemaphoreType.DMA
    frame = pl.pallas_call(
        functools.partial(kernel, counts, chunks),
        out_shape=jax.ShapeDtypeStruct((channels, band, LANES), f32),
        in_specs=[pl.BlockSpec(memory_space=pltpu.SMEM), pl.BlockSpec(memory_space=pl.ANY)],
        out_specs=pl.BlockSpec(memory_space=pl.ANY),
        scratch_shapes=[
            pltpu.VMEM((nx, channels, band * LANES), images.dtype),
            pltpu.VMEM((nx - 1, channels, band, LANES), images.dtype),
            pltpu.VMEM((nx - 1, channels, band, LANES), images.dtype),
            pltpu.VMEM((channels, band, LANES), f32),
            pltpu.VMEM((ny - 1, channels, band // ny, LANES), f32),
            pltpu.VMEM((channels, band // ny, LANES), f32),
            pltpu.VMEM((nz - 1, channels, band // (ny * nz), LANES), f32),
            pltpu.VMEM((channels, band // (ny * nz), LANES), f32),
            pltpu.VMEM((band // chunks * 8, LANES), f32),
            dma((chunks, nx)),
            dma((chunks, nx - 1)), dma((chunks, nx - 1)),
            dma((chunks, ny - 1)), dma((chunks, ny - 1)),
            dma((chunks, nz - 1)), dma((chunks, nz - 1)),
            dma((chunks, ny * nz)), dma((chunks, ny * nz)),
            dma((chunks,)),
        ],
        compiler_params=pltpu.CompilerParams(
            collective_id=0, has_side_effects=True, vmem_limit_bytes=60 * 1024 * 1024),
    )(order, images)
    return frame.reshape(channels, band * LANES)


def solution(mesh):
    counts = tuple(mesh.shape[a] for a in AXES)
    return jax.shard_map(
        functools.partial(per_device, counts), mesh=mesh,
        in_specs=(P(AXES, None, None), P()), out_specs=P(None, "gx"), check_vma=False)
```
